32 devices in a mesh: shard: 8 (over z, x), grp: 4 (over y, core).
Axes of the slice: x: 2, y: 2, z: 4, core: 2. Of those that a mesh axis runs over, the one named last changes fastest.
Arguments:
- table_t: bfloat16 [100, 622592], P(None, ('shard', 'grp')), may hold values from -6 to 6
- req_rows: int32 [1024, 128], P(('shard', 'grp')), may hold values from 0 to 19455
- count1: int32 [1024], P(('shard', 'grp')), may hold values from 1 to 128, as said below
- frontier_list: int32 [11, 32768], P(None, ('shard', 'grp')), may hold values from 0 to 4095, as said below
- req2_rows: int32 [1024, 128], P(('shard', 'grp')), may hold values from 0 to 1023
- count2: int32 [1024], P(('shard', 'grp')), may hold values from 1 to 128, as said below
- seed_list: int32 [16, 8192], P(None, ('shard', 'grp')), may hold values from 0 to 4095, as said below
- w1_self: bfloat16 [256, 100], replicated, may hold values from -0.625 to 0.625
- w1_neigh: bfloat16 [256, 100], replicated, may hold values from -1.25 to 1.25
- bias1: float32 [256], replicated, may hold values from -3 to 3
- w2_self: bfloat16 [47, 256], replicated, may hold values from -0.375 to 0.375
- w2_neigh: bfloat16 [47, 256], replicated, may hold values from -0.75 to 0.75
- bias2: float32 [47], replicated, may hold values from -3 to 3
Outputs:
- logits: float32 [47, 8192], P(None, ('shard', 'grp'))
The draws below stay inside these ranges and needn't reach their ends.
Inputs may be any that keep to these rules, and one draw needn't show every extreme that they name: count1[r * 32 + o] counts the live slots of the block that device r asks of device o; in every draw some devices are asked for 128 rows by every device. `frontier_list`: every entry o * 128 + j names a live slot (j below count1 of that block) of the asking device. count2[r * 32 + o] counts the live slots of the block that device r asks of device o; in every draw some devices are asked for 128 rows by every device. `seed_list`: every entry o * 128 + j names a live slot (j below count2 of that block) of the asking device.
All inputs are finite; a program needn't handle non-finite values.
Results may differ from the reference program's by a relative error of at most 0.0029.
Values may be sent and summed in bfloat16 or wider, within the bound.
A program may use at most 64 MiB of HBM per device.

```python
import jax
import jax.numpy as jnp
from jax import lax

F = 100
H = 256
C = 47
K1 = 15
K2 = 10
ROWS_DEV = 19456
FRONT_DEV = 1024
SEED_DEV = 256
CAP = 128
CAP2 = 128
NODES = 622592
PAIRS = 1024
N_SHARD = 8
N_GRP = 4
DEVICES = 32


def counts_table(key, capacity):
    first_key, second_key = jax.random.split(key)
    base = jax.random.randint(first_key, (DEVICES, DEVICES), max(1, capacity // 8), capacity // 2 + 1)
    hottest = jax.random.permutation(second_key, DEVICES)[:max(1, DEVICES // 16)]
    is_hot = jnp.any(jnp.arange(DEVICES)[:, None] == hottest[None, :], axis=1)
    return jnp.where(is_hot[None, :], capacity, base).astype(jnp.int32)


def slot_table(key, counts, capacity, entries, per_device):
    first_key, second_key = jax.random.split(key)
    owners = jax.random.randint(first_key, (entries, DEVICES * per_device), 0, DEVICES)
    askers = jnp.broadcast_to((jnp.arange(DEVICES * per_device) // per_device)[None, :], owners.shape)
    live_count = counts[askers, owners]
    offset = jax.random.randint(second_key, owners.shape, 0, 1 << 30) % live_count
    return (owners * capacity + offset).astype(jnp.int32)


def draw_count1(key, part):
    return counts_table(jax.random.fold_in(key, 101), CAP).reshape(-1)


def draw_frontier_list(key, part):
    counts = counts_table(jax.random.fold_in(key, 101), CAP)
    return slot_table(jax.random.fold_in(key, 102), counts, CAP, K2 + 1, FRONT_DEV)


def draw_count2(key, part):
    return counts_table(jax.random.fold_in(key, 201), CAP2).reshape(-1)


def draw_seed_list(key, part):
    counts = counts_table(jax.random.fold_in(key, 201), CAP2)
    return slot_table(jax.random.fold_in(key, 202), counts, CAP2, K1 + 1, SEED_DEV)


def with_ends(values, rng, smallest, top_value):
    shape = values.shape
    index_at = [jax.random.randint(jax.random.fold_in(rng, axis), (), 0, shape[axis]) for axis in range(len(shape))]
    values = values.at[tuple(index_at)].set(smallest)
    longest = shape.index(max(shape))
    index_at[longest] = (index_at[longest] + 1) % shape[longest]
    return values.at[tuple(index_at)].set(top_value)


def block_levels(stream_key, shape, cuts, smallest, largest):
    level, own = 1.0, jax.random.fold_in(stream_key, 6)
    for axis_at, parts in cuts:
        steps = jnp.exp(jax.random.uniform(jax.random.fold_in(own, axis_at), (parts,), jnp.float32, smallest / len(cuts), largest / len(cuts)))
        level = level * jnp.repeat(steps, shape[axis_at] // parts).reshape([-1 if axis == axis_at else 1 for axis in range(len(shape))])
    return level


def gaussian(key, extent, width, most, cuts=(), kind=jnp.bfloat16):
    values = jax.random.normal(key, extent, jnp.float32) * width
    if len(cuts) > 0:
        values = block_levels(key, extent, cuts, -0.22, 0.18) * values
    return jnp.clip(values, min=-most, max=most).astype(kind)


def setup_inputs(seed: int = 0) -> dict:
    streams_of = jax.random.split(jax.random.key(seed), 14)
    table_t = gaussian(streams_of[0], (F, NODES), 1.0, 6.0, ((1, 32),))
    req_rows = with_ends(jax.random.randint(streams_of[1], (PAIRS, CAP), 0, ROWS_DEV), jax.random.fold_in(streams_of[1], 1), 0, ROWS_DEV - 1).astype(jnp.int32)
    count1 = draw_count1(jax.random.fold_in(streams_of[13], 71), 0)
    frontier_list = draw_frontier_list(jax.random.fold_in(streams_of[13], 71), 0)
    req2_rows = with_ends(jax.random.randint(streams_of[4], (PAIRS, CAP2), 0, FRONT_DEV), jax.random.fold_in(streams_of[4], 1), 0, FRONT_DEV - 1).astype(jnp.int32)
    count2 = draw_count2(jax.random.fold_in(streams_of[13], 71), 0)
    seed_list = draw_seed_list(jax.random.fold_in(streams_of[13], 71), 0)
    w1_self = gaussian(streams_of[7], (H, F), F ** -0.5, 0.625)
    w1_neigh = gaussian(streams_of[8], (H, F), (F // 4) ** -0.5, 1.25)
    bias1 = gaussian(streams_of[9], (H,), 0.5, 3.0, (), jnp.float32)
    w2_self = gaussian(streams_of[10], (C, H), H ** -0.5, 0.375)
    w2_neigh = gaussian(streams_of[11], (C, H), (H // 4) ** -0.5, 0.75)
    bias2 = gaussian(streams_of[12], (C,), 0.5, 3.0, (), jnp.float32)
    return dict(table_t=table_t, req_rows=req_rows, count1=count1, frontier_list=frontier_list, req2_rows=req2_rows, count2=count2, seed_list=seed_list, w1_self=w1_self, w1_neigh=w1_neigh, bias1=bias1, w2_self=w2_self, w2_neigh=w2_neigh, bias2=bias2)


def reference(table_t, req_rows, count1, frontier_list, req2_rows, count2, seed_list, w1_self, w1_neigh, bias1, w2_self, w2_neigh, bias2):
    devices = N_SHARD * N_GRP
    table_base = (jnp.arange(devices, dtype=jnp.int32) * ROWS_DEV)[:, None]
    front_base = (jnp.arange(devices, dtype=jnp.int32) * FRONT_DEV)[:, None]
    asked_one = req_rows.reshape(devices, devices, CAP)
    counts_one = count1.reshape(devices, devices)
    lists_one = frontier_list.reshape(K2 + 1, devices, FRONT_DEV).transpose(1, 0, 2)

    def layer_one(args):
        wanted, counts, picks = args
        columns = jnp.take(table_t, (wanted + table_base).reshape(-1).astype(jnp.int32), axis=1)
        is_live = (jnp.arange(CAP, dtype=jnp.int32)[None, :] < counts[:, None]).reshape(-1)
        columns = jnp.where(is_live[None, :], columns, jnp.zeros((), columns.dtype))
        picked = jnp.take(columns, picks.reshape(-1), axis=1).reshape(F, K2 + 1, FRONT_DEV)
        summed = (jnp.sum(picked[:, 1:].astype(jnp.float32), axis=1) / K2).astype(jnp.bfloat16)
        preact = jnp.dot(w1_self, picked[:, 0], preferred_element_type=jnp.float32)
        preact = preact + jnp.dot(w1_neigh, summed, preferred_element_type=jnp.float32) + bias1[:, None]
        return jax.nn.relu(preact).astype(jnp.bfloat16)

    hidden = lax.map(layer_one, (asked_one, counts_one, lists_one))
    hidden = hidden.transpose(1, 0, 2).reshape(H, devices * FRONT_DEV)
    asked_two = req2_rows.reshape(devices, devices, CAP2)
    counts_two = count2.reshape(devices, devices)
    lists_two = seed_list.reshape(K1 + 1, devices, SEED_DEV).transpose(1, 0, 2)

    def layer_two(args):
        wanted, counts, picks = args
        columns = jnp.take(hidden, (wanted + front_base).reshape(-1).astype(jnp.int32), axis=1)
        is_live = (jnp.arange(CAP2, dtype=jnp.int32)[None, :] < counts[:, None]).reshape(-1)
        columns = jnp.where(is_live[None, :], columns, jnp.zeros((), columns.dtype))
        picked = jnp.take(columns, picks.reshape(-1), axis=1).reshape(H, K1 + 1, SEED_DEV)
        near = jnp.sum(picked[:, 1:].astype(jnp.float32), axis=1) / K1
        result = jnp.dot(w2_self, picked[:, 0], preferred_element_type=jnp.float32)
        result = result + jnp.dot(w2_neigh.astype(jnp.float32), near, precision=lax.Precision.HIGHEST, preferred_element_type=jnp.float32)
        return result + bias2[:, None]

    logits = lax.map(layer_two, (asked_two, counts_two, lists_two))
    return logits.transpose(1, 0, 2).reshape(C, devices * SEED_DEV)
```

```python
import functools

import jax
import jax.numpy as jnp
from jax import lax
from jax.experimental import pallas as pl
from jax.experimental.pallas import tpu as pltpu
from jax.sharding import PartitionSpec as P

AXES = ("shard", "grp")
LANES = 128
MIB = 1024 * 1024
MATRIX_LIMIT = 4 * MIB
VMEM_ALL = pl.BlockSpec(memory_space=pltpu.VMEM)
SMEM_ALL = pl.BlockSpec(memory_space=pltpu.SMEM)


def params(mib=48, **extra):
    return pltpu.CompilerParams(vmem_limit_bytes=mib * MIB, **extra)


def cost(flops, moved):
    return pl.CostEstimate(flops=int(flops), bytes_accessed=int(moved), transcendentals=0)


def local_rows(values, base, span):
    local = values - base
    inside = jnp.logical_and(local >= 0, local < span)
    return jnp.where(inside, local, -1).astype(jnp.float32)


def iota_groups(span):
    base = lax.broadcasted_iota(jnp.int32, (16, LANES), 0)
    return [(base + 16 * g).astype(jnp.float32).astype(jnp.bfloat16) for g in range(span // 16)]


def count_kernel(list_ref, own_ref, near_ref):
    span = own_ref.shape[0]
    local = local_rows(list_ref[...], pl.program_id(0) * span, span)
    groups = iota_groups(span)
    one, zero = jnp.ones((), jnp.bfloat16), jnp.zeros((), jnp.bfloat16)
    for c in range(own_ref.shape[1] // LANES):
        cols = slice(c * LANES, (c + 1) * LANES)
        counts = [jnp.zeros((16, LANES), jnp.bfloat16) for _ in groups]
        for k in range(list_ref.shape[0]):
            row = jnp.broadcast_to(local[k : k + 1, cols], (16, LANES)).astype(jnp.bfloat16)
            for g, ids in enumerate(groups):
                hit = jnp.where(row == ids, one, zero)
                if k == 0:
                    own_ref[16 * g : 16 * g + 16, cols] = hit
                else:
                    counts[g] = counts[g] + hit
        for g in range(len(groups)):
            near_ref[16 * g : 16 * g + 16, cols] = counts[g]


def count_matrices(picks, slots, cap):
    entries, nodes = picks.shape
    out = jax.ShapeDtypeStruct((slots, nodes), jnp.bfloat16)
    return pl.pallas_call(
        count_kernel,
        grid=(slots // cap,),
        in_specs=[pl.BlockSpec((entries, nodes), lambda o: (0, 0))],
        out_specs=[pl.BlockSpec((cap, nodes), lambda o: (o, 0))] * 2,
        out_shape=[out, out],
        compiler_params=params(),
        cost_estimate=cost(entries * slots * nodes * 4, slots * nodes * 4),
    )(picks)


def onehot_kernel(ids_ref, out_ref):
    groups = iota_groups(LANES)
    one, zero = jnp.ones((), jnp.bfloat16), jnp.zeros((), jnp.bfloat16)
    wanted = ids_ref[pl.ds(pl.program_id(0), 1), :]
    for c in range(out_ref.shape[1] // LANES):
        cols = slice(c * LANES, (c + 1) * LANES)
        for b in range(out_ref.shape[0] // LANES):
            local = local_rows(wanted[:, cols], b * LANES, LANES)
            row = jnp.broadcast_to(local, (16, LANES)).astype(jnp.bfloat16)
            for g, ids in enumerate(groups):
                at = b * LANES + 16 * g
                out_ref[at : at + 16, cols] = jnp.where(row == ids, one, zero)


def onehot_matrix(ids, nodes):
    devices, cap = ids.shape
    return pl.pallas_call(
        onehot_kernel,
        grid=(devices,),
        in_specs=[pl.BlockSpec((devices, cap), lambda o: (0, 0))],
        out_specs=pl.BlockSpec((nodes, cap), lambda o: (0, o)),
        out_shape=jax.ShapeDtypeStruct((nodes, devices * cap), jnp.bfloat16),
        compiler_params=params(),
        cost_estimate=cost(nodes * devices * cap * 4, nodes * devices * cap * 2),
    )(ids)


def rows_kernel(table_ref, out_ref):
    out_ref[...] = table_ref[...].astype(jnp.float32).T


def table_rows(table_t):
    width, rows = table_t.shape
    step = next(s for s in (1024, 512, 256, 128) if rows % s == 0)
    return pl.pallas_call(
        rows_kernel,
        grid=(rows // step,),
        in_specs=[pl.BlockSpec((width, step), lambda i: (0, i))],
        out_specs=pl.BlockSpec((step, width), lambda i: (i, 0)),
        out_shape=jax.ShapeDtypeStruct((rows, width), jnp.float32),
        compiler_params=params(),
        cost_estimate=cost(rows * width * 64, rows * width * 6),
    )(table_t)


def gather_kernel(ids_ref, rows_ref, out_ref, block):
    cap = ids_ref.shape[1]

    def one_asker(asker, carry):
        for j in range(cap):
            block[j : j + 1, :] = rows_ref[pl.ds(ids_ref[asker, j], 1), :]
        out_ref[asker] = block[...].T.astype(jnp.bfloat16)
        return carry

    lax.fori_loop(0, ids_ref.shape[0], one_asker, 0)


def gather_columns(ids, rows):
    devices, cap = ids.shape
    width = rows.shape[1]
    return pl.pallas_call(
        gather_kernel,
        in_specs=[SMEM_ALL, VMEM_ALL],
        out_specs=VMEM_ALL,
        out_shape=jax.ShapeDtypeStruct((devices, width, cap), jnp.bfloat16),
        scratch_shapes=[pltpu.VMEM((cap, width), jnp.float32)],
        compiler_params=params(),
        cost_estimate=cost(devices * cap * width * 64, rows.size * 4),
    )(ids, rows)


def lay_side_by_side(counts_ref, blocks_ref, flat):
    devices, width, cap = blocks_ref.shape
    slot = lax.broadcasted_iota(jnp.int32, (width, cap), 1)

    def one(o, carry):
        block = blocks_ref[o].astype(jnp.float32)
        live = jnp.where(slot < counts_ref[o], block, 0.0)
        flat[:, pl.ds(pl.multiple_of(o * cap, cap), cap)] = live.astype(jnp.bfloat16)
        return carry

    lax.fori_loop(0, devices, one, 0)


def dot32(a, b):
    return jnp.dot(a, b, preferred_element_type=jnp.float32)


def front_kernel(
    fanout,
    counts_ref,
    got_ref,
    own_ref,
    near_ref,
    onehot_ref,
    w1s_ref,
    w1n_ref,
    bias_ref,
    w2_ref,
    out_ref,
    flat,
    payload,
):
    lay_side_by_side(counts_ref, got_ref, flat)
    nodes = own_ref.shape[1]
    wide = 256

    def nodes_chunk(c, carry):
        cols = pl.ds(pl.multiple_of(c * wide, wide), wide)
        own = dot32(flat[...], own_ref[:, cols]).astype(jnp.bfloat16)
        summed = (dot32(flat[...], near_ref[:, cols]) / fanout).astype(jnp.bfloat16)
        preact = dot32(w1s_ref[...], own) + dot32(w1n_ref[...], summed) + bias_ref[...]
        hidden = jnp.maximum(preact, 0.0).astype(jnp.bfloat16)
        payload[:, cols] = dot32(w2_ref[...], hidden).astype(jnp.bfloat16)
        return carry

    lax.fori_loop(0, nodes // wide, nodes_chunk, 0)
    cap = out_ref.shape[2]
    pair = 2

    def askers(p, carry):
        cols = pl.ds(pl.multiple_of(p * pair * cap, pair * cap), pair * cap)
        chosen = dot32(payload[...], onehot_ref[:, cols]).astype(jnp.bfloat16)
        for h in range(pair):
            out_ref[p * pair + h] = chosen[:, h * cap : (h + 1) * cap]
        return carry

    lax.fori_loop(0, out_ref.shape[0] // pair, askers, 0)


def front_payload(counts, got, own, near, onehot, w1s, w1n, bias1, w2, fanout):
    devices, width, cap = got.shape
    slots, nodes = own.shape
    return pl.pallas_call(
        functools.partial(front_kernel, float(fanout)),
        in_specs=[SMEM_ALL] + [VMEM_ALL] * 8,
        out_specs=VMEM_ALL,
        out_shape=jax.ShapeDtypeStruct((devices, w2.shape[0], cap), jnp.bfloat16),
        scratch_shapes=[
            pltpu.VMEM((width, slots), jnp.bfloat16),
            pltpu.VMEM((w2.shape[0], nodes), jnp.bfloat16),
        ],
        compiler_params=params(),
        cost_estimate=cost(slots * nodes * 600, slots * nodes * 6),
    )(counts, got, own, near, onehot, w1s, w1n, bias1, w2)


def seed_kernel(fanout, classes, counts_ref, got_ref, own_ref, near_ref, bias_ref, out_ref, flat):
    lay_side_by_side(counts_ref, got_ref, flat)
    half = flat.shape[0] // 2
    mine = dot32(flat[:half], own_ref[...])
    near = dot32(flat[half:], near_ref[...]) / fanout
    out_ref[...] = (mine + near)[:classes] + bias_ref[...]


def seed_logits(counts, got, own, near, bias2, fanout):
    classes = bias2.shape[0]
    devices, width, cap = got.shape
    slots, seeds = own.shape
    return pl.pallas_call(
        functools.partial(seed_kernel, float(fanout), classes),
        in_specs=[SMEM_ALL] + [VMEM_ALL] * 4,
        out_specs=VMEM_ALL,
        out_shape=jax.ShapeDtypeStruct((classes, seeds), jnp.float32),
        scratch_shapes=[pltpu.VMEM((width, slots), jnp.bfloat16)],
        compiler_params=params(),
        cost_estimate=cost(slots * seeds * 400, slots * seeds * 4),
    )(counts, got, own, near, bias2)


def exchange(blocks):
    return lax.all_to_all(blocks, AXES, split_axis=0, concat_axis=0, tiled=True)


def stacked_w2(w2_self, w2_neigh):
    classes = w2_self.shape[0]
    half = -(-classes // 16) * 16
    pad = ((0, half - classes), (0, 0))
    return jnp.concatenate([jnp.pad(w2_self, pad), jnp.pad(w2_neigh, pad)], axis=0)


def mask_rows(received, counts, capacity):
    is_live = (jnp.arange(capacity, dtype=jnp.int32)[None, :] < counts[:, None]).reshape(-1)
    flat = received.reshape(-1, received.shape[-1])
    return jnp.where(is_live[:, None], flat, jnp.zeros((), flat.dtype))


def right_product(rows, weight):
    return lax.dot_general(
        rows, weight, (((1,), (1,)), ((), ())), preferred_element_type=jnp.float32
    )


def take_body(
    table_t,
    req_rows,
    count1,
    frontier_list,
    req2_rows,
    count2,
    seed_list,
    w1_self,
    w1_neigh,
    bias1,
    w2_self,
    w2_neigh,
    bias2,
):
    feat_width = table_t.shape[0]
    capacity = req_rows.shape[1]
    table_rows = table_t.T
    picked_rows = jnp.take(
        table_rows,
        lax.all_to_all(req_rows, AXES, split_axis=0, concat_axis=0, tiled=True),
        axis=0,
    )
    received = lax.all_to_all(
        picked_rows, AXES, split_axis=0, concat_axis=0, tiled=True
    )
    flat = mask_rows(received, count1, capacity)
    fanout_two = frontier_list.shape[0] - 1
    front_nodes = frontier_list.shape[1]
    picked = jnp.take(flat, frontier_list.reshape(-1), axis=0).reshape(
        fanout_two + 1, front_nodes, feat_width
    )
    summed = (jnp.sum(picked[1:].astype(jnp.float32), axis=0) / fanout_two).astype(jnp.bfloat16)
    preact = right_product(picked[0], w1_self) + right_product(summed, w1_neigh) + bias1[None, :]
    hidden_rows = jax.nn.relu(preact).astype(jnp.bfloat16)
    cap_two = req2_rows.shape[1]
    payload = jnp.concatenate(
        [right_product(hidden_rows, w2_self), right_product(hidden_rows, w2_neigh)], axis=1
    )
    chosen = jnp.take(
        payload,
        lax.all_to_all(req2_rows, AXES, split_axis=0, concat_axis=0, tiled=True),
        axis=0,
    )
    got_back = lax.all_to_all(chosen, AXES, split_axis=0, concat_axis=0, tiled=True)
    flat_two = mask_rows(got_back, count2, cap_two)
    fanout_one = seed_list.shape[0] - 1
    seed_nodes = seed_list.shape[1]
    picked_two = jnp.take(flat_two, seed_list.reshape(-1), axis=0).reshape(
        fanout_one + 1, seed_nodes, flat_two.shape[1]
    )
    classes = w2_self.shape[0]
    near = jnp.sum(picked_two[1:, :, classes:], axis=0) / fanout_one
    logits = (picked_two[0, :, :classes] + near).T + bias2[:, None]
    return logits


def body(
    table_t,
    req_rows,
    count1,
    frontier_list,
    req2_rows,
    count2,
    seed_list,
    w1_self,
    w1_neigh,
    bias1,
    w2_self,
    w2_neigh,
    bias2,
):
    devices, cap = req_rows.shape
    cap_two = req2_rows.shape[1]
    nodes = frontier_list.shape[1]
    if devices * max(cap, cap_two) * nodes > MATRIX_LIMIT:
        return take_body(
            table_t,
            req_rows,
            count1,
            frontier_list,
            req2_rows,
            count2,
            seed_list,
            w1_self,
            w1_neigh,
            bias1,
            w2_self,
            w2_neigh,
            bias2,
        )
    asked = exchange(jnp.concatenate([req_rows, req2_rows], axis=1))
    rows = table_rows(table_t)
    picked = gather_columns(asked[:, :cap], rows)
    got = exchange(picked)
    fan_two = frontier_list.shape[0] - 1
    fan_one = seed_list.shape[0] - 1
    frontier_list, seed_list, asked_two, _ = lax.optimization_barrier(
        (frontier_list, seed_list, asked[:, cap:], picked)
    )
    own, near = count_matrices(frontier_list, devices * cap, cap)
    onehot = onehot_matrix(asked_two, nodes)
    seed_own, seed_near = count_matrices(seed_list, devices * cap_two, cap_two)
    payload = front_payload(
        count1,
        got,
        own,
        near,
        onehot,
        w1_self,
        w1_neigh,
        bias1[:, None],
        stacked_w2(w2_self, w2_neigh),
        fan_two,
    )
    got_two = exchange(payload)
    return seed_logits(count2, got_two, seed_own, seed_near, bias2[:, None], fan_one)


def solution(mesh):
    in_specs = (
        P(None, AXES),
        P(AXES, None),
        P(AXES),
        P(None, AXES),
        P(AXES, None),
        P(AXES),
        P(None, AXES),
        P(),
        P(),
        P(),
        P(),
        P(),
        P(),
    )
    return jax.shard_map(
        body, mesh=mesh, in_specs=in_specs, out_specs=P(None, AXES), check_vma=False
    )
```

```python
import functools

import jax
import jax.numpy as jnp
from jax import lax
from jax.experimental import pallas as pl
from jax.experimental.pallas import tpu as pltpu
from jax.sharding import PartitionSpec as P

AXES = ("shard", "grp")
LANES = 128
MIB = 1024 * 1024
MATRIX_LIMIT = 4 * MIB
VMEM_ALL = pl.BlockSpec(memory_space=pltpu.VMEM)
SMEM_ALL = pl.BlockSpec(memory_space=pltpu.SMEM)


def tall(row, span):
    few = jnp.broadcast_to(row, (16, row.shape[1])).astype(jnp.bfloat16)
    return jnp.concatenate([few] * (span // 16), axis=0)


def local_rows(values, base, span):
    local = values - base
    inside = jnp.logical_and(local >= 0, local < span)
    return jnp.where(inside, local, -1).astype(jnp.float32)


def hits(row, span):
    ids = lax.broadcasted_iota(jnp.int32, (span, row.shape[1]), 0)
    ids = ids.astype(jnp.float32).astype(jnp.bfloat16)
    return jnp.where(tall(row, span) == ids, jnp.ones((), jnp.bfloat16), jnp.zeros((), jnp.bfloat16))


def tile(i, size=LANES):
    return pl.ds(pl.multiple_of(i * size, size), size)


def count_slots(list_ref, own_ref, near_ref, cap):
    entries, nodes = list_ref.shape
    across = nodes // LANES

    def one(i, carry):
        owner, cols = i // across, tile(i % across)
        at = tile(owner, cap)
        local = local_rows(list_ref[:, cols], owner * cap, cap)
        own_ref[at, cols] = hits(local[0:1], cap)
        total = hits(local[1:2], cap)
        for k in range(2, entries):
            total = total + hits(local[k : k + 1], cap)
        near_ref[at, cols] = total
        return carry

    lax.fori_loop(0, own_ref.shape[0] // cap * across, one, 0)


def onehot_slots(ids_ref, out_ref):
    nodes = out_ref.shape[0]
    devices, _, cap = ids_ref.shape

    def one(asker, carry):
        wanted = ids_ref[asker]
        for b in range(nodes // LANES):
            out_ref[b * LANES : (b + 1) * LANES, tile(asker, cap)] = hits(
                local_rows(wanted, b * LANES, LANES), LANES
            )
        return carry

    lax.fori_loop(0, devices, one, 0)


def lay_side_by_side(counts_ref, blocks_ref, flat):
    devices, width, cap = blocks_ref.shape
    slot = lax.broadcasted_iota(jnp.int32, (width, cap), 1)

    def one(o, carry):
        live = jnp.where(slot < counts_ref[o], blocks_ref[o].astype(jnp.float32), 0.0)
        flat[:, tile(o, cap)] = live.astype(jnp.bfloat16)
        return carry

    lax.fori_loop(0, devices, one, 0)


def dot32(a, b):
    return jnp.dot(a, b, preferred_element_type=jnp.float32)


def whole_kernel(
    grp,
    table_ref,
    req_ref,
    req2_ref,
    count1_ref,
    count2_ref,
    front_ref,
    seed_ref,
    w1s_ref,
    w1n_ref,
    bias1_ref,
    w2_ref,
    bias2_ref,
    out_ref,
    asked,
    asked2,
    ids,
    rows,
    block,
    send,
    got,
    own,
    near,
    onehot,
    seed_own,
    seed_near,
    flat,
    payload,
    send2,
    got2,
    flat2,
    local_sem,
    sems,
):
    devices, _, cap = req_ref.shape
    me = lax.axis_index(AXES[0]) * grp + lax.axis_index(AXES[1])

    def partner(t):
        return (me + t) % devices

    def copy(what, src, dst, peer):
        return pltpu.make_async_remote_copy(
            src_ref=src.at[peer],
            dst_ref=dst.at[me],
            send_sem=sems.at[2 * what, peer],
            recv_sem=sems.at[2 * what + 1, me],
            device_id=(peer // grp, peer % grp),
            device_id_type=pl.DeviceIdType.MESH,
        )

    def wait_all(what, src, dst):
        def one(t, carry):
            peer = partner(t)
            pltpu.make_async_remote_copy(
                src_ref=src.at[peer],
                dst_ref=dst.at[peer],
                send_sem=sems.at[2 * what, peer],
                recv_sem=sems.at[2 * what + 1, peer],
                device_id=(peer // grp, peer % grp),
                device_id_type=pl.DeviceIdType.MESH,
            ).wait()
            return carry

        lax.fori_loop(1, devices, one, 0)

    barrier = pltpu.get_barrier_semaphore()

    def greet(t, carry):
        peer = partner(t)
        pl.semaphore_signal(
            barrier,
            inc=1,
            device_id=(peer // grp, peer % grp),
            device_id_type=pl.DeviceIdType.MESH,
        )
        return carry

    lax.fori_loop(1, devices, greet, 0)
    pl.semaphore_wait(barrier, devices - 1)

    def ask(t, carry):
        copy(0, req_ref, asked, partner(t)).start()
        copy(1, req2_ref, asked2, partner(t)).start()
        return carry

    lax.fori_loop(1, devices, ask, 0)
    asked[me] = req_ref[me]
    asked2[me] = req2_ref[me]

    step = 4 * LANES if rows.shape[0] % (4 * LANES) == 0 else LANES

    def transpose(i, carry):
        rows[tile(i, step), :] = table_ref[:, tile(i, step)].T.astype(jnp.float32)
        return carry

    lax.fori_loop(0, rows.shape[0] // step, transpose, 0)
    wait_all(0, req_ref, asked)
    wait_all(1, req2_ref, asked2)
    to_scalars = pltpu.make_async_copy(asked, ids, local_sem)
    to_scalars.start()
    to_scalars.wait()

    def pick(asker):
        for j in range(cap):
            block[j : j + 1, :] = rows[pl.ds(ids[asker, 0, j], 1), :]
        return block[...].T.astype(jnp.bfloat16)

    got[me] = pick(me)
    send[partner(1)] = pick(partner(1))

    def pick_and_send(t, carry):
        send[partner(t)] = pick(partner(t))
        copy(2, send, got, partner(t - 1)).start()
        return carry

    lax.fori_loop(2, devices, pick_and_send, 0)
    onehot_slots(asked2, onehot)
    copy(2, send, got, partner(devices - 1)).start()
    count_slots(front_ref, own, near, cap)
    wait_all(2, send, got)

    lay_side_by_side(count1_ref, got, flat)
    wide = 2 * LANES
    fan_two, fan_one = float(front_ref.shape[0] - 1), float(seed_ref.shape[0] - 1)

    def nodes_chunk(c, carry):
        cols = tile(c, wide)
        mine = dot32(flat[...], own[:, cols]).astype(jnp.bfloat16)
        summed = (dot32(flat[...], near[:, cols]) / fan_two).astype(jnp.bfloat16)
        preact = dot32(w1s_ref[...], mine) + dot32(w1n_ref[...], summed) + bias1_ref[...]
        hidden = jnp.maximum(preact, 0.0).astype(jnp.bfloat16)
        payload[:, cols] = dot32(w2_ref[...], hidden).astype(jnp.bfloat16)
        return carry

    lax.fori_loop(0, own.shape[1] // wide, nodes_chunk, 0)
    cap_two = req2_ref.shape[2]

    def chosen(asker):
        return dot32(payload[...], onehot[:, tile(asker, cap_two)]).astype(jnp.bfloat16)

    got2[me] = chosen(me)
    send2[partner(1)] = chosen(partner(1))

    def choose_and_send(t, carry):
        send2[partner(t)] = chosen(partner(t))
        copy(3, send2, got2, partner(t - 1)).start()
        return carry

    lax.fori_loop(2, devices, choose_and_send, 0)
    bias2 = bias2_ref[...]
    copy(3, send2, got2, partner(devices - 1)).start()
    count_slots(seed_ref, seed_own, seed_near, cap_two)
    wait_all(3, send2, got2)
    lay_side_by_side(count2_ref, got2, flat2)
    half = flat2.shape[0] // 2
    self_term = dot32(flat2[:half], seed_own[...])
    near_term = dot32(flat2[half:], seed_near[...]) / fan_one
    out_ref[...] = (self_term + near_term)[: out_ref.shape[0]] + bias2


def stacked_w2(w2_self, w2_neigh):
    classes = w2_self.shape[0]
    half = -(-classes // 16) * 16
    pad = ((0, half - classes), (0, 0))
    return jnp.concatenate([jnp.pad(w2_self, pad), jnp.pad(w2_neigh, pad)], axis=0)


def mask_rows(received, counts, capacity):
    is_live = (jnp.arange(capacity, dtype=jnp.int32)[None, :] < counts[:, None]).reshape(-1)
    flat = received.reshape(-1, received.shape[-1])
    return jnp.where(is_live[:, None], flat, jnp.zeros((), flat.dtype))


def right_product(rows, weight):
    return lax.dot_general(
        rows, weight, (((1,), (1,)), ((), ())), preferred_element_type=jnp.float32
    )


def take_body(
    table_t,
    req_rows,
    count1,
    frontier_list,
    req2_rows,
    count2,
    seed_list,
    w1_self,
    w1_neigh,
    bias1,
    w2_self,
    w2_neigh,
    bias2,
):
    feat_width = table_t.shape[0]
    capacity = req_rows.shape[1]
    table_rows = table_t.T
    picked_rows = jnp.take(
        table_rows,
        lax.all_to_all(req_rows, AXES, split_axis=0, concat_axis=0, tiled=True),
        axis=0,
    )
    received = lax.all_to_all(
        picked_rows, AXES, split_axis=0, concat_axis=0, tiled=True
    )
    flat = mask_rows(received, count1, capacity)
    fanout_two = frontier_list.shape[0] - 1
    front_nodes = frontier_list.shape[1]
    picked = jnp.take(flat, frontier_list.reshape(-1), axis=0).reshape(
        fanout_two + 1, front_nodes, feat_width
    )
    summed = (jnp.sum(picked[1:].astype(jnp.float32), axis=0) / fanout_two).astype(jnp.bfloat16)
    preact = right_product(picked[0], w1_self) + right_product(summed, w1_neigh) + bias1[None, :]
    hidden_rows = jax.nn.relu(preact).astype(jnp.bfloat16)
    cap_two = req2_rows.shape[1]
    payload = jnp.concatenate(
        [right_product(hidden_rows, w2_self), right_product(hidden_rows, w2_neigh)], axis=1
    )
    chosen = jnp.take(
        payload,
        lax.all_to_all(req2_rows, AXES, split_axis=0, concat_axis=0, tiled=True),
        axis=0,
    )
    got_back = lax.all_to_all(chosen, AXES, split_axis=0, concat_axis=0, tiled=True)
    flat_two = mask_rows(got_back, count2, cap_two)
    fanout_one = seed_list.shape[0] - 1
    seed_nodes = seed_list.shape[1]
    picked_two = jnp.take(flat_two, seed_list.reshape(-1), axis=0).reshape(
        fanout_one + 1, seed_nodes, flat_two.shape[1]
    )
    classes = w2_self.shape[0]
    near = jnp.sum(picked_two[1:, :, classes:], axis=0) / fanout_one
    logits = (picked_two[0, :, :classes] + near).T + bias2[:, None]
    return logits


def body(
    table_t,
    req_rows,
    count1,
    frontier_list,
    req2_rows,
    count2,
    seed_list,
    w1_self,
    w1_neigh,
    bias1,
    w2_self,
    w2_neigh,
    bias2,
):
    devices, cap = req_rows.shape
    cap_two = req2_rows.shape[1]
    nodes = frontier_list.shape[1]
    if devices * max(cap, cap_two) * nodes > MATRIX_LIMIT:
        return take_body(
            table_t,
            req_rows,
            count1,
            frontier_list,
            req2_rows,
            count2,
            seed_list,
            w1_self,
            w1_neigh,
            bias1,
            w2_self,
            w2_neigh,
            bias2,
        )
    width, table_rows = table_t.shape
    seeds = seed_list.shape[1]
    w2 = stacked_w2(w2_self, w2_neigh)
    slots, slots_two = devices * cap, devices * cap_two
    bf16, f32, i32 = jnp.bfloat16, jnp.float32, jnp.int32
    return pl.pallas_call(
        functools.partial(whole_kernel, lax.axis_size(AXES[1])),
        in_specs=[VMEM_ALL] * 3 + [SMEM_ALL] * 2 + [VMEM_ALL] * 7,
        out_specs=VMEM_ALL,
        out_shape=jax.ShapeDtypeStruct((w2_self.shape[0], seeds), f32),
        scratch_shapes=[
            pltpu.VMEM((devices, 1, cap), i32),
            pltpu.VMEM((devices, 1, cap_two), i32),
            pltpu.SMEM((devices, 1, cap), i32),
            pltpu.VMEM((table_rows, width), f32),
            pltpu.VMEM((cap, width), f32),
            pltpu.VMEM((devices, width, cap), bf16),
            pltpu.VMEM((devices, width, cap), bf16),
            pltpu.VMEM((slots, nodes), bf16),
            pltpu.VMEM((slots, nodes), bf16),
            pltpu.VMEM((nodes, slots_two), bf16),
            pltpu.VMEM((slots_two, seeds), bf16),
            pltpu.VMEM((slots_two, seeds), bf16),
            pltpu.VMEM((width, slots), bf16),
            pltpu.VMEM((w2.shape[0], nodes), bf16),
            pltpu.VMEM((devices, w2.shape[0], cap_two), bf16),
            pltpu.VMEM((devices, w2.shape[0], cap_two), bf16),
            pltpu.VMEM((w2.shape[0], slots_two), bf16),
            pltpu.SemaphoreType.DMA,
            pltpu.SemaphoreType.DMA((8, devices)),
        ],
        compiler_params=pltpu.CompilerParams(
            vmem_limit_bytes=63 * MIB, collective_id=0, has_side_effects=True
        ),
    )(
        table_t,
        req_rows[:, None, :],
        req2_rows[:, None, :],
        count1,
        count2,
        frontier_list,
        seed_list,
        w1_self,
        w1_neigh,
        bias1[:, None],
        w2,
        bias2[:, None],
    )


def solution(mesh):
    in_specs = (
        P(None, AXES),
        P(AXES, None),
        P(AXES),
        P(None, AXES),
        P(AXES, None),
        P(AXES),
        P(None, AXES),
        P(),
        P(),
        P(),
        P(),
        P(),
        P(),
    )
    return jax.shard_map(
        body, mesh=mesh, in_specs=in_specs, out_specs=P(None, AXES), check_vma=False
    )
```

```python
import functools

import jax
import jax.numpy as jnp
from jax import lax
from jax.experimental import pallas as pl
from jax.experimental.pallas import tpu as pltpu
from jax.sharding import PartitionSpec as P

AXES = ("shard", "grp")
LANES = 128
MIB = 1024 * 1024
MATRIX_LIMIT = 4 * MIB
VMEM_ALL = pl.BlockSpec(memory_space=pltpu.VMEM)
SMEM_ALL = pl.BlockSpec(memory_space=pltpu.SMEM)


def tall(row, span):
    few = jnp.broadcast_to(row, (16, row.shape[1])).astype(jnp.bfloat16)
    return jnp.concatenate([few] * (span // 16), axis=0)


def local_rows(values, base, span):
    local = values - base
    inside = jnp.logical_and(local >= 0, local < span)
    return jnp.where(inside, local, -1).astype(jnp.float32)


def hits(row, span):
    ids = lax.broadcasted_iota(jnp.int32, (span, row.shape[1]), 0)
    ids = ids.astype(jnp.float32).astype(jnp.bfloat16)
    return jnp.where(tall(row, span) == ids, jnp.ones((), jnp.bfloat16), jnp.zeros((), jnp.bfloat16))


def tile(i, size=LANES):
    return pl.ds(pl.multiple_of(i * size, size), size)


def count_slots(list_ref, own_ref, near_ref, cap, first, last):
    entries, nodes = list_ref.shape
    across = nodes // LANES

    def one(i, carry):
        owner, cols = i // across, tile(i % across)
        at = tile(owner, cap)
        local = local_rows(list_ref[:, cols], owner * cap, cap)
        own_ref[at, cols] = hits(local[0:1], cap)
        total = hits(local[1:2], cap)
        for k in range(2, entries):
            total = total + hits(local[k : k + 1], cap)
        near_ref[at, cols] = total
        return carry

    lax.fori_loop(first * across, last * across, one, 0)


def onehot_slots(ids_ref, out_ref):
    nodes = out_ref.shape[0]
    devices, _, cap = ids_ref.shape

    def one(asker, carry):
        wanted = ids_ref[asker]
        for b in range(nodes // LANES):
            out_ref[b * LANES : (b + 1) * LANES, tile(asker, cap)] = hits(
                local_rows(wanted, b * LANES, LANES), LANES
            )
        return carry

    lax.fori_loop(0, devices, one, 0)


def lay_side_by_side(counts_ref, blocks_ref, flat):
    devices, width, cap = blocks_ref.shape
    slot = lax.broadcasted_iota(jnp.int32, (width, cap), 1)

    def one(o, carry):
        live = jnp.where(slot < counts_ref[o], blocks_ref[o].astype(jnp.float32), 0.0)
        flat[:, tile(o, cap)] = live.astype(jnp.bfloat16)
        return carry

    lax.fori_loop(0, devices, one, 0)


def dot32(a, b):
    return jnp.dot(a, b, preferred_element_type=jnp.float32)


def whole_kernel(
    grp,
    table_ref,
    req_ref,
    req2_ref,
    count1_ref,
    count2_ref,
    front_ref,
    seed_ref,
    w1s_ref,
    w1n_ref,
    bias1_ref,
    w2s_ref,
    w2n_ref,
    out_ref,
    table,
    w1s,
    w1n,
    w2,
    asked,
    asked2,
    ids,
    rows,
    block,
    send,
    got,
    own,
    near,
    onehot,
    seed_own,
    seed_near,
    flat,
    payload,
    send2,
    got2,
    flat2,
    local_sem,
    table_sem,
    sems,
):
    devices, _, cap = req_ref.shape
    me = lax.axis_index(AXES[0]) * grp + lax.axis_index(AXES[1])

    def partner(t):
        return (me + t) % devices

    def copy(what, src, dst, peer):
        return pltpu.make_async_remote_copy(
            src_ref=src.at[peer],
            dst_ref=dst.at[me],
            send_sem=sems.at[2 * what, peer],
            recv_sem=sems.at[2 * what + 1, me],
            device_id=(peer // grp, peer % grp),
            device_id_type=pl.DeviceIdType.MESH,
        )

    def wait_all(what, src, dst):
        def one(t, carry):
            peer = partner(t)
            pltpu.make_async_remote_copy(
                src_ref=src.at[peer],
                dst_ref=dst.at[peer],
                send_sem=sems.at[2 * what, peer],
                recv_sem=sems.at[2 * what + 1, peer],
                device_id=(peer // grp, peer % grp),
                device_id_type=pl.DeviceIdType.MESH,
            ).wait()
            return carry

        lax.fori_loop(1, devices, one, 0)

    load = pltpu.make_async_copy(table_ref, table, table_sem)
    load.start()
    barrier = pltpu.get_barrier_semaphore()

    def greet(t, carry):
        peer = partner(t)
        pl.semaphore_signal(
            barrier,
            inc=1,
            device_id=(peer // grp, peer % grp),
            device_id_type=pl.DeviceIdType.MESH,
        )
        return carry

    lax.fori_loop(1, devices, greet, 0)
    early = devices // 8
    count_slots(front_ref, own, near, cap, 0, early)
    pl.semaphore_wait(barrier, devices - 1)

    def ask(t, carry):
        copy(0, req_ref, asked, partner(t)).start()
        copy(1, req2_ref, asked2, partner(t)).start()
        return carry

    lax.fori_loop(1, devices, ask, 0)
    asked[me] = req_ref[me]
    asked2[me] = req2_ref[me]
    w1s[...] = w1s_ref[...].T
    w1n[...] = w1n_ref[...].T
    classes, half = w2s_ref.shape[0], w2.shape[0] // 2
    w2[...] = jnp.zeros_like(w2)
    w2[:classes] = w2s_ref[...]
    w2[half : half + classes] = w2n_ref[...]
    bias1 = jnp.broadcast_to(bias1_ref[...], (8, bias1_ref.shape[1])).T[:, :1]
    load.wait()

    step = 4 * LANES if rows.shape[0] % (4 * LANES) == 0 else LANES

    def transpose(i, carry):
        rows[tile(i, step), :] = table[:, tile(i, step)].T.astype(jnp.float32)
        return carry

    lax.fori_loop(0, rows.shape[0] // step, transpose, 0)
    wait_all(0, req_ref, asked)
    wait_all(1, req2_ref, asked2)
    to_scalars = pltpu.make_async_copy(asked, ids, local_sem)
    to_scalars.start()
    to_scalars.wait()

    def pick(asker):
        for j in range(cap):
            block[j : j + 1, :] = rows[pl.ds(ids[asker, 0, j], 1), :]
        return block[...].T.astype(jnp.bfloat16)

    got[me] = pick(me)
    send[partner(1)] = pick(partner(1))

    def pick_and_send(t, carry):
        send[partner(t)] = pick(partner(t))
        copy(2, send, got, partner(t - 1)).start()
        return carry

    lax.fori_loop(2, devices, pick_and_send, 0)
    onehot_slots(asked2, onehot)
    copy(2, send, got, partner(devices - 1)).start()
    count_slots(front_ref, own, near, cap, early, devices)
    wait_all(2, send, got)

    lay_side_by_side(count1_ref, got, flat)
    wide = 2 * LANES
    fan_two, fan_one = float(front_ref.shape[0] - 1), float(seed_ref.shape[0] - 1)

    def nodes_chunk(c, carry):
        cols = tile(c, wide)
        mine = dot32(flat[...], own[:, cols]).astype(jnp.bfloat16)
        summed = (dot32(flat[...], near[:, cols]) / fan_two).astype(jnp.bfloat16)
        preact = dot32(w1s[...], mine) + dot32(w1n[...], summed) + bias1
        hidden = jnp.maximum(preact, 0.0).astype(jnp.bfloat16)
        payload[:, cols] = dot32(w2[...], hidden).astype(jnp.bfloat16)
        return carry

    lax.fori_loop(0, own.shape[1] // wide, nodes_chunk, 0)
    cap_two = req2_ref.shape[2]

    def chosen(asker):
        return dot32(payload[...], onehot[:, tile(asker, cap_two)]).astype(jnp.bfloat16)

    got2[me] = chosen(me)
    send2[partner(1)] = chosen(partner(1))

    def choose_and_send(t, carry):
        send2[partner(t)] = chosen(partner(t))
        copy(3, send2, got2, partner(t - 1)).start()
        return carry

    lax.fori_loop(2, devices, choose_and_send, 0)
    copy(3, send2, got2, partner(devices - 1)).start()
    count_slots(seed_ref, seed_own, seed_near, cap_two, 0, devices)
    wait_all(3, send2, got2)
    lay_side_by_side(count2_ref, got2, flat2)
    self_term = dot32(flat2[:half], seed_own[...])
    near_term = dot32(flat2[half:], seed_near[...]) / fan_one
    out_ref[...] = (self_term + near_term)[:classes]


def mask_rows(received, counts, capacity):
    is_live = (jnp.arange(capacity, dtype=jnp.int32)[None, :] < counts[:, None]).reshape(-1)
    flat = received.reshape(-1, received.shape[-1])
    return jnp.where(is_live[:, None], flat, jnp.zeros((), flat.dtype))


def right_product(rows, weight):
    return lax.dot_general(
        rows, weight, (((1,), (1,)), ((), ())), preferred_element_type=jnp.float32
    )


def take_body(
    table_t,
    req_rows,
    count1,
    frontier_list,
    req2_rows,
    count2,
    seed_list,
    w1_self,
    w1_neigh,
    bias1,
    w2_self,
    w2_neigh,
    bias2,
):
    feat_width = table_t.shape[0]
    capacity = req_rows.shape[1]
    table_rows = table_t.T
    picked_rows = jnp.take(
        table_rows,
        lax.all_to_all(req_rows, AXES, split_axis=0, concat_axis=0, tiled=True),
        axis=0,
    )
    received = lax.all_to_all(
        picked_rows, AXES, split_axis=0, concat_axis=0, tiled=True
    )
    flat = mask_rows(received, count1, capacity)
    fanout_two = frontier_list.shape[0] - 1
    front_nodes = frontier_list.shape[1]
    picked = jnp.take(flat, frontier_list.reshape(-1), axis=0).reshape(
        fanout_two + 1, front_nodes, feat_width
    )
    summed = (jnp.sum(picked[1:].astype(jnp.float32), axis=0) / fanout_two).astype(jnp.bfloat16)
    preact = right_product(picked[0], w1_self) + right_product(summed, w1_neigh) + bias1[None, :]
    hidden_rows = jax.nn.relu(preact).astype(jnp.bfloat16)
    cap_two = req2_rows.shape[1]
    payload = jnp.concatenate(
        [right_product(hidden_rows, w2_self), right_product(hidden_rows, w2_neigh)], axis=1
    )
    chosen = jnp.take(
        payload,
        lax.all_to_all(req2_rows, AXES, split_axis=0, concat_axis=0, tiled=True),
        axis=0,
    )
    got_back = lax.all_to_all(chosen, AXES, split_axis=0, concat_axis=0, tiled=True)
    flat_two = mask_rows(got_back, count2, cap_two)
    fanout_one = seed_list.shape[0] - 1
    seed_nodes = seed_list.shape[1]
    picked_two = jnp.take(flat_two, seed_list.reshape(-1), axis=0).reshape(
        fanout_one + 1, seed_nodes, flat_two.shape[1]
    )
    classes = w2_self.shape[0]
    near = jnp.sum(picked_two[1:, :, classes:], axis=0) / fanout_one
    logits = (picked_two[0, :, :classes] + near).T + bias2[:, None]
    return logits


def body(
    table_t,
    req_rows,
    count1,
    frontier_list,
    req2_rows,
    count2,
    seed_list,
    w1_self,
    w1_neigh,
    bias1,
    w2_self,
    w2_neigh,
    bias2,
):
    devices, cap = req_rows.shape
    cap_two = req2_rows.shape[1]
    nodes = frontier_list.shape[1]
    if devices * max(cap, cap_two) * nodes > MATRIX_LIMIT:
        return take_body(
            table_t,
            req_rows,
            count1,
            frontier_list,
            req2_rows,
            count2,
            seed_list,
            w1_self,
            w1_neigh,
            bias1,
            w2_self,
            w2_neigh,
            bias2,
        )
    width, table_rows = table_t.shape
    seeds = seed_list.shape[1]
    hidden_width, classes = w1_self.shape[0], w2_self.shape[0]
    rows_two = 2 * (-(-classes // 16) * 16)
    slots, slots_two = devices * cap, devices * cap_two
    bf16, f32, i32 = jnp.bfloat16, jnp.float32, jnp.int32
    logits = pl.pallas_call(
        functools.partial(whole_kernel, lax.axis_size(AXES[1])),
        in_specs=[pl.BlockSpec(memory_space=pl.ANY)] + [VMEM_ALL] * 2 + [SMEM_ALL] * 2 + [VMEM_ALL] * 7,
        out_specs=VMEM_ALL,
        out_shape=jax.ShapeDtypeStruct((classes, seeds), f32),
        scratch_shapes=[
            pltpu.VMEM((width, table_rows), bf16),
            pltpu.VMEM((hidden_width, width), bf16),
            pltpu.VMEM((hidden_width, width), bf16),
            pltpu.VMEM((rows_two, hidden_width), bf16),
            pltpu.VMEM((devices, 1, cap), i32),
            pltpu.VMEM((devices, 1, cap_two), i32),
            pltpu.SMEM((devices, 1, cap), i32),
            pltpu.VMEM((table_rows, width), f32),
            pltpu.VMEM((cap, width), f32),
            pltpu.VMEM((devices, width, cap), bf16),
            pltpu.VMEM((devices, width, cap), bf16),
            pltpu.VMEM((slots, nodes), bf16),
            pltpu.VMEM((slots, nodes), bf16),
            pltpu.VMEM((nodes, slots_two), bf16),
            pltpu.VMEM((slots_two, seeds), bf16),
            pltpu.VMEM((slots_two, seeds), bf16),
            pltpu.VMEM((width, slots), bf16),
            pltpu.VMEM((rows_two, nodes), bf16),
            pltpu.VMEM((devices, rows_two, cap_two), bf16),
            pltpu.VMEM((devices, rows_two, cap_two), bf16),
            pltpu.VMEM((rows_two, slots_two), bf16),
            pltpu.SemaphoreType.DMA,
            pltpu.SemaphoreType.DMA,
            pltpu.SemaphoreType.DMA((8, devices)),
        ],
        compiler_params=pltpu.CompilerParams(
            vmem_limit_bytes=63 * MIB, collective_id=0, has_side_effects=True
        ),
    )(
        table_t,
        req_rows[:, None, :],
        req2_rows[:, None, :],
        count1,
        count2,
        frontier_list,
        seed_list,
        w1_self.T,
        w1_neigh.T,
        bias1[None, :],
        w2_self,
        w2_neigh,
    )
    return logits + bias2[:, None]


def solution(mesh):
    in_specs = (
        P(None, AXES),
        P(AXES, None),
        P(AXES),
        P(None, AXES),
        P(AXES, None),
        P(AXES),
        P(None, AXES),
        P(),
        P(),
        P(),
        P(),
        P(),
        P(),
    )
    return jax.shard_map(
        body, mesh=mesh, in_specs=in_specs, out_specs=P(None, AXES), check_vma=False
    )
```

```python
import functools

import jax
import jax.numpy as jnp
from jax import lax
from jax.experimental import pallas as pl
from jax.experimental.pallas import tpu as pltpu
from jax.sharding import PartitionSpec as P

AXES = ("shard", "grp")
LANES = 128
MIB = 1024 * 1024
MATRIX_LIMIT = 4 * MIB
VMEM_ALL = pl.BlockSpec(memory_space=pltpu.VMEM)
SMEM_ALL = pl.BlockSpec(memory_space=pltpu.SMEM)


def tall(row, span):
    few = jnp.broadcast_to(row, (16, row.shape[1])).astype(jnp.bfloat16)
    return jnp.concatenate([few] * (span // 16), axis=0)


def local_rows(values, base, span):
    local = values - base
    inside = jnp.logical_and(local >= 0, local < span)
    return jnp.where(inside, local, -1).astype(jnp.float32)


def places(span):
    ids = lax.broadcasted_iota(jnp.int32, (span, LANES), 0)
    return ids.astype(jnp.float32).astype(jnp.bfloat16)


def hits(row, ids):
    one, zero = jnp.ones((), jnp.bfloat16), jnp.zeros((), jnp.bfloat16)
    return jnp.where(tall(row, ids.shape[0]) == ids, one, zero)


def tile(i, size=LANES):
    return pl.ds(pl.multiple_of(i * size, size), size)


def count_tile(list_ref, own_ref, near_ref, ids, owner, c):
    cap = ids.shape[0]
    cols, at = tile(c), tile(owner, cap)
    local = local_rows(list_ref[:, cols], owner * cap, cap)
    own_ref[at, cols] = hits(local[0:1], ids)
    total = hits(local[1:2], ids)
    for k in range(2, list_ref.shape[0]):
        total = total + hits(local[k : k + 1], ids)
    near_ref[at, cols] = total


def count_slots(list_ref, own_ref, near_ref, ids, first, last):
    across = list_ref.shape[1] // LANES

    def one(i, carry):
        count_tile(list_ref, own_ref, near_ref, ids, i // across, i % across)
        return carry

    lax.fori_loop(first * across, last * across, one, 0)


def lay_side_by_side(counts_ref, blocks_ref, flat):
    devices, width, cap = blocks_ref.shape
    slot = lax.broadcasted_iota(jnp.int32, (width, cap), 1)

    def one(o, carry):
        live = jnp.where(slot < counts_ref[o], blocks_ref[o].astype(jnp.float32), 0.0)
        flat[:, tile(o, cap)] = live.astype(jnp.bfloat16)
        return carry

    lax.fori_loop(0, devices, one, 0)


def dot32(a, b):
    return jnp.dot(a, b, preferred_element_type=jnp.float32)


def whole_kernel(
    grp,
    table_ref,
    req_ref,
    req2_ref,
    count1_ref,
    count2_ref,
    front_ref,
    seed_ref,
    w1s_ref,
    w1n_ref,
    bias1_ref,
    w2s_ref,
    w2n_ref,
    out_ref,
    table,
    w1s,
    w1n,
    w2,
    asked,
    asked2,
    ids,
    rows,
    block,
    send,
    got,
    own,
    near,
    seed_own,
    seed_near,
    flat,
    payload,
    send2,
    got2,
    flat2,
    local_sem,
    table_sem,
    sems,
):
    devices, _, cap = req_ref.shape
    cap_two = req2_ref.shape[2]
    me = lax.axis_index(AXES[0]) * grp + lax.axis_index(AXES[1])

    def partner(t):
        return (me + t) % devices

    def copy(what, src, dst, peer):
        return pltpu.make_async_remote_copy(
            src_ref=src.at[peer],
            dst_ref=dst.at[me],
            send_sem=sems.at[2 * what, peer],
            recv_sem=sems.at[2 * what + 1, me],
            device_id=(peer // grp, peer % grp),
            device_id_type=pl.DeviceIdType.MESH,
        )

    def wait_all(what, src, dst):
        def one(t, carry):
            peer = partner(t)
            pltpu.make_async_remote_copy(
                src_ref=src.at[peer],
                dst_ref=dst.at[peer],
                send_sem=sems.at[2 * what, peer],
                recv_sem=sems.at[2 * what + 1, peer],
                device_id=(peer // grp, peer % grp),
                device_id_type=pl.DeviceIdType.MESH,
            ).wait()
            return carry

        lax.fori_loop(1, devices, one, 0)

    load = pltpu.make_async_copy(table_ref, table, table_sem)
    load.start()
    barrier = pltpu.get_barrier_semaphore()

    def greet(t, carry):
        peer = partner(t)
        pl.semaphore_signal(
            barrier,
            inc=1,
            device_id=(peer // grp, peer % grp),
            device_id_type=pl.DeviceIdType.MESH,
        )
        return carry

    lax.fori_loop(1, devices, greet, 0)
    marks, marks2, node_marks = places(cap), places(cap_two), places(LANES)
    early = 2
    count_slots(front_ref, own, near, marks, 0, early)
    pl.semaphore_wait(barrier, devices - 1)

    def ask(t, carry):
        copy(0, req_ref, asked, partner(t)).start()
        copy(1, req2_ref, asked2, partner(t)).start()
        return carry

    lax.fori_loop(1, devices, ask, 0)
    asked[me] = req_ref[me]
    asked2[me] = req2_ref[me]
    w1s[...] = w1s_ref[...].T
    w1n[...] = w1n_ref[...].T
    classes, half = w2s_ref.shape[0], w2.shape[0] // 2
    w2[...] = jnp.zeros_like(w2)
    w2[:classes] = w2s_ref[...]
    w2[half : half + classes] = w2n_ref[...]
    bias1 = jnp.broadcast_to(bias1_ref[...], (8, bias1_ref.shape[1])).T[:, :1]
    load.wait()

    step = 4 * LANES if rows.shape[0] % (4 * LANES) == 0 else LANES

    def transpose(i, carry):
        rows[tile(i, step), :] = table[:, tile(i, step)].T.astype(jnp.float32)
        return carry

    lax.fori_loop(0, rows.shape[0] // step, transpose, 0)
    wait_all(0, req_ref, asked)
    wait_all(1, req2_ref, asked2)
    to_scalars = pltpu.make_async_copy(asked, ids, local_sem)
    to_scalars.start()
    to_scalars.wait()

    across = front_ref.shape[1] // LANES
    share = -(-cap // across)

    def pick(asker, owner=None):
        for c in range(across):
            for j in range(c * share, min(cap, (c + 1) * share)):
                block[j : j + 1, :] = rows[pl.ds(ids[asker, 0, j], 1), :]
            if owner is not None:
                count_tile(front_ref, own, near, marks, owner, c)
        return block[...].T.astype(jnp.bfloat16)

    got[me] = pick(me)
    send[partner(1)] = pick(partner(1))

    def pick_and_send(t, carry):
        send[partner(t)] = pick(partner(t), t)
        copy(2, send, got, partner(t - 1)).start()
        return carry

    lax.fori_loop(early, devices, pick_and_send, 0)
    count_slots(seed_ref, seed_own, seed_near, marks2, 0, 1)
    copy(2, send, got, partner(devices - 1)).start()
    wait_all(2, send, got)

    lay_side_by_side(count1_ref, got, flat)
    wide = 2 * LANES
    fan_two, fan_one = float(front_ref.shape[0] - 1), float(seed_ref.shape[0] - 1)

    def nodes_chunk(c, carry):
        cols = tile(c, wide)
        mine = dot32(flat[...], own[:, cols]).astype(jnp.bfloat16)
        summed = (dot32(flat[...], near[:, cols]) / fan_two).astype(jnp.bfloat16)
        preact = dot32(w1s[...], mine) + dot32(w1n[...], summed) + bias1
        hidden = jnp.maximum(preact, 0.0).astype(jnp.bfloat16)
        payload[:, cols] = dot32(w2[...], hidden).astype(jnp.bfloat16)
        return carry

    lax.fori_loop(0, own.shape[1] // wide, nodes_chunk, 0)

    def chosen(asker):
        wanted = asked2[asker]
        select = [
            hits(local_rows(wanted, b * LANES, LANES), node_marks)
            for b in range(payload.shape[1] // LANES)
        ]
        return dot32(payload[...], jnp.concatenate(select, axis=0)).astype(jnp.bfloat16)

    got2[me] = chosen(me)
    send2[partner(1)] = chosen(partner(1))

    def choose_and_send(t, carry):
        send2[partner(t)] = chosen(partner(t))
        copy(3, send2, got2, partner(t - 1)).start()
        return carry

    lax.fori_loop(2, devices, choose_and_send, 0)
    count_slots(seed_ref, seed_own, seed_near, marks2, 1, 2)
    copy(3, send2, got2, partner(devices - 1)).start()
    count_slots(seed_ref, seed_own, seed_near, marks2, 2, devices)
    wait_all(3, send2, got2)
    lay_side_by_side(count2_ref, got2, flat2)
    self_term = dot32(flat2[:half], seed_own[...])
    near_term = dot32(flat2[half:], seed_near[...]) / fan_one
    out_ref[...] = (self_term + near_term)[:classes]


def mask_rows(received, counts, capacity):
    is_live = (jnp.arange(capacity, dtype=jnp.int32)[None, :] < counts[:, None]).reshape(-1)
    flat = received.reshape(-1, received.shape[-1])
    return jnp.where(is_live[:, None], flat, jnp.zeros((), flat.dtype))


def right_product(rows, weight):
    return lax.dot_general(
        rows, weight, (((1,), (1,)), ((), ())), preferred_element_type=jnp.float32
    )


def take_body(
    table_t,
    req_rows,
    count1,
    frontier_list,
    req2_rows,
    count2,
    seed_list,
    w1_self,
    w1_neigh,
    bias1,
    w2_self,
    w2_neigh,
    bias2,
):
    feat_width = table_t.shape[0]
    capacity = req_rows.shape[1]
    table_rows = table_t.T
    picked_rows = jnp.take(
        table_rows,
        lax.all_to_all(req_rows, AXES, split_axis=0, concat_axis=0, tiled=True),
        axis=0,
    )
    received = lax.all_to_all(
        picked_rows, AXES, split_axis=0, concat_axis=0, tiled=True
    )
    flat = mask_rows(received, count1, capacity)
    fanout_two = frontier_list.shape[0] - 1
    front_nodes = frontier_list.shape[1]
    picked = jnp.take(flat, frontier_list.reshape(-1), axis=0).reshape(
        fanout_two + 1, front_nodes, feat_width
    )
    summed = (jnp.sum(picked[1:].astype(jnp.float32), axis=0) / fanout_two).astype(jnp.bfloat16)
    preact = right_product(picked[0], w1_self) + right_product(summed, w1_neigh) + bias1[None, :]
    hidden_rows = jax.nn.relu(preact).astype(jnp.bfloat16)
    cap_two = req2_rows.shape[1]
    payload = jnp.concatenate(
        [right_product(hidden_rows, w2_self), right_product(hidden_rows, w2_neigh)], axis=1
    )
    chosen = jnp.take(
        payload,
        lax.all_to_all(req2_rows, AXES, split_axis=0, concat_axis=0, tiled=True),
        axis=0,
    )
    got_back = lax.all_to_all(chosen, AXES, split_axis=0, concat_axis=0, tiled=True)
    flat_two = mask_rows(got_back, count2, cap_two)
    fanout_one = seed_list.shape[0] - 1
    seed_nodes = seed_list.shape[1]
    picked_two = jnp.take(flat_two, seed_list.reshape(-1), axis=0).reshape(
        fanout_one + 1, seed_nodes, flat_two.shape[1]
    )
    classes = w2_self.shape[0]
    near = jnp.sum(picked_two[1:, :, classes:], axis=0) / fanout_one
    logits = (picked_two[0, :, :classes] + near).T + bias2[:, None]
    return logits


def body(
    table_t,
    req_rows,
    count1,
    frontier_list,
    req2_rows,
    count2,
    seed_list,
    w1_self,
    w1_neigh,
    bias1,
    w2_self,
    w2_neigh,
    bias2,
):
    devices, cap = req_rows.shape
    cap_two = req2_rows.shape[1]
    nodes = frontier_list.shape[1]
    if devices * max(cap, cap_two) * nodes > MATRIX_LIMIT:
        return take_body(
            table_t,
            req_rows,
            count1,
            frontier_list,
            req2_rows,
            count2,
            seed_list,
            w1_self,
            w1_neigh,
            bias1,
            w2_self,
            w2_neigh,
            bias2,
        )
    width, table_rows = table_t.shape
    seeds = seed_list.shape[1]
    hidden_width, classes = w1_self.shape[0], w2_self.shape[0]
    rows_two = 2 * (-(-classes // 16) * 16)
    slots, slots_two = devices * cap, devices * cap_two
    bf16, f32, i32 = jnp.bfloat16, jnp.float32, jnp.int32
    logits = pl.pallas_call(
        functools.partial(whole_kernel, lax.axis_size(AXES[1])),
        in_specs=[pl.BlockSpec(memory_space=pl.ANY)] + [VMEM_ALL] * 2 + [SMEM_ALL] * 2 + [VMEM_ALL] * 7,
        out_specs=VMEM_ALL,
        out_shape=jax.ShapeDtypeStruct((classes, seeds), f32),
        scratch_shapes=[
            pltpu.VMEM((width, table_rows), bf16),
            pltpu.VMEM((hidden_width, width), bf16),
            pltpu.VMEM((hidden_width, width), bf16),
            pltpu.VMEM((rows_two, hidden_width), bf16),
            pltpu.VMEM((devices, 1, cap), i32),
            pltpu.VMEM((devices, 1, cap_two), i32),
            pltpu.SMEM((devices, 1, cap), i32),
            pltpu.VMEM((table_rows, width), f32),
            pltpu.VMEM((cap, width), f32),
            pltpu.VMEM((devices, width, cap), bf16),
            pltpu.VMEM((devices, width, cap), bf16),
            pltpu.VMEM((slots, nodes), bf16),
            pltpu.VMEM((slots, nodes), bf16),
            pltpu.VMEM((slots_two, seeds), bf16),
            pltpu.VMEM((slots_two, seeds), bf16),
            pltpu.VMEM((width, slots), bf16),
            pltpu.VMEM((rows_two, nodes), bf16),
            pltpu.VMEM((devices, rows_two, cap_two), bf16),
            pltpu.VMEM((devices, rows_two, cap_two), bf16),
            pltpu.VMEM((rows_two, slots_two), bf16),
            pltpu.SemaphoreType.DMA,
            pltpu.SemaphoreType.DMA,
            pltpu.SemaphoreType.DMA((8, devices)),
        ],
        compiler_params=pltpu.CompilerParams(
            vmem_limit_bytes=63 * MIB, collective_id=0, has_side_effects=True
        ),
    )(
        table_t,
        req_rows[:, None, :],
        req2_rows[:, None, :],
        count1,
        count2,
        frontier_list,
        seed_list,
        w1_self.T,
        w1_neigh.T,
        bias1[None, :],
        w2_self,
        w2_neigh,
    )
    return logits + bias2[:, None]


def solution(mesh):
    in_specs = (
        P(None, AXES),
        P(AXES, None),
        P(AXES),
        P(None, AXES),
        P(AXES, None),
        P(AXES),
        P(None, AXES),
        P(),
        P(),
        P(),
        P(),
        P(),
        P(),
    )
    return jax.shard_map(
        body, mesh=mesh, in_specs=in_specs, out_specs=P(None, AXES), check_vma=False
    )
```

```python
import functools

import jax
import jax.numpy as jnp
from jax import lax
from jax.experimental import pallas as pl
from jax.experimental.pallas import tpu as pltpu
from jax.sharding import PartitionSpec as P

AXES = ("shard", "grp")
LANES = 128
MIB = 1024 * 1024
MATRIX_LIMIT = 4 * MIB
VMEM_ALL = pl.BlockSpec(memory_space=pltpu.VMEM)
SMEM_ALL = pl.BlockSpec(memory_space=pltpu.SMEM)


def tall(row, span):
    few = jnp.broadcast_to(row, (16, row.shape[1])).astype(jnp.bfloat16)
    return jnp.concatenate([few] * (span // 16), axis=0)


def local_rows(values, base, span):
    local = values - base
    inside = jnp.logical_and(local >= 0, local < span)
    return jnp.where(inside, local, -1).astype(jnp.float32)


def places(span):
    ids = lax.broadcasted_iota(jnp.int32, (span, LANES), 0)
    return ids.astype(jnp.float32).astype(jnp.bfloat16)


def hits(row, ids):
    one, zero = jnp.ones((), jnp.bfloat16), jnp.zeros((), jnp.bfloat16)
    return jnp.where(tall(row, ids.shape[0]) == ids, one, zero)


def tile(i, size=LANES):
    return pl.ds(pl.multiple_of(i * size, size), size)


def count_tile(list_ref, own_ref, near_ref, ids, owner, c, place):
    cap = ids.shape[0]
    cols, at = tile(c), tile(place, cap)
    local = local_rows(list_ref[:, cols], owner * cap, cap)
    own_ref[at, cols] = hits(local[0:1], ids)
    total = hits(local[1:2], ids)
    for k in range(2, list_ref.shape[0]):
        total = total + hits(local[k : k + 1], ids)
    near_ref[at, cols] = total


def count_slots(list_ref, own_ref, near_ref, ids, first, last, owner_of=lambda place: place):
    across = list_ref.shape[1] // LANES

    def one(i, carry):
        place = i // across
        count_tile(list_ref, own_ref, near_ref, ids, owner_of(place), i % across, place)
        return carry

    lax.fori_loop(first * across, last * across, one, 0)


def lay_side_by_side(counts_ref, blocks_ref, flat, first, last, owner_of=lambda place: place):
    _, width, cap = blocks_ref.shape
    slot = lax.broadcasted_iota(jnp.int32, (width, cap), 1)

    def one(place, carry):
        o = owner_of(place)
        live = jnp.where(slot < counts_ref[o], blocks_ref[o].astype(jnp.float32), 0.0)
        flat[:, tile(place, cap)] = live.astype(jnp.bfloat16)
        return carry

    lax.fori_loop(first, last, one, 0)


def dot32(a, b):
    return jnp.dot(a, b, preferred_element_type=jnp.float32)


def whole_kernel(
    grp,
    table_ref,
    req_ref,
    req2_ref,
    count1_ref,
    count2_ref,
    front_ref,
    seed_ref,
    w1s_ref,
    w1n_ref,
    bias1_ref,
    w2s_ref,
    w2n_ref,
    out_ref,
    table,
    w1s,
    w1n,
    w2,
    asked,
    asked2,
    ids,
    rows,
    block,
    send,
    got,
    own,
    near,
    seed_own,
    seed_near,
    flat,
    sums,
    payload,
    send2,
    got2,
    flat2,
    local_sem,
    table_sem,
    sems,
):
    devices, _, cap = req_ref.shape
    cap_two = req2_ref.shape[2]
    me = lax.axis_index(AXES[0]) * grp + lax.axis_index(AXES[1])

    def partner(t):
        return (me + t) % devices

    def copy(what, src, dst, peer):
        return pltpu.make_async_remote_copy(
            src_ref=src.at[peer],
            dst_ref=dst.at[me],
            send_sem=sems.at[2 * what, peer],
            recv_sem=sems.at[2 * what + 1, me],
            device_id=(peer // grp, peer % grp),
            device_id_type=pl.DeviceIdType.MESH,
        )

    def wait_all(what, src, dst, first=1, last=devices):
        def one(t, carry):
            peer = partner(t)
            pltpu.make_async_remote_copy(
                src_ref=src.at[peer],
                dst_ref=dst.at[peer],
                send_sem=sems.at[2 * what, peer],
                recv_sem=sems.at[2 * what + 1, peer],
                device_id=(peer // grp, peer % grp),
                device_id_type=pl.DeviceIdType.MESH,
            ).wait()
            return carry

        lax.fori_loop(first, last, one, 0)

    load = pltpu.make_async_copy(table_ref, table, table_sem)
    load.start()
    barrier = pltpu.get_barrier_semaphore()

    def greet(t, carry):
        peer = partner(t)
        pl.semaphore_signal(
            barrier,
            inc=1,
            device_id=(peer // grp, peer % grp),
            device_id_type=pl.DeviceIdType.MESH,
        )
        return carry

    lax.fori_loop(1, devices, greet, 0)
    marks, marks2, node_marks = places(cap), places(cap_two), places(LANES)
    early = 2
    count_slots(front_ref, own, near, marks, 0, early, partner)
    pl.semaphore_wait(barrier, devices - 1)

    def ask(t, carry):
        copy(0, req_ref, asked, partner(t)).start()
        copy(1, req2_ref, asked2, partner(t)).start()
        return carry

    lax.fori_loop(1, devices, ask, 0)
    asked[me] = req_ref[me]
    asked2[me] = req2_ref[me]
    w1s[...] = w1s_ref[...].T
    w1n[...] = w1n_ref[...].T
    classes, half = w2s_ref.shape[0], w2.shape[0] // 2
    w2[...] = jnp.zeros_like(w2)
    w2[:classes] = w2s_ref[...]
    w2[half : half + classes] = w2n_ref[...]
    bias1 = jnp.broadcast_to(bias1_ref[...], (8, bias1_ref.shape[1])).T[:, :1]
    load.wait()

    step = 4 * LANES if rows.shape[0] % (4 * LANES) == 0 else LANES

    def transpose(i, carry):
        rows[tile(i, step), :] = table[:, tile(i, step)].T.astype(jnp.float32)
        return carry

    lax.fori_loop(0, rows.shape[0] // step, transpose, 0)
    wait_all(0, req_ref, asked)
    wait_all(1, req2_ref, asked2)
    to_scalars = pltpu.make_async_copy(asked, ids, local_sem)
    to_scalars.start()
    to_scalars.wait()

    across = front_ref.shape[1] // LANES
    share = -(-cap // across)

    def pick(asker, place=None):
        for c in range(across):
            for j in range(c * share, min(cap, (c + 1) * share)):
                block[j : j + 1, :] = rows[pl.ds(ids[asker, 0, j], 1), :]
            if place is not None:
                count_tile(front_ref, own, near, marks, partner(place), c, place)
        return block[...].T.astype(jnp.bfloat16)

    got[me] = pick(me)
    send[partner(1)] = pick(partner(1))

    def pick_and_send(t, carry):
        send[partner(t)] = pick(partner(t), t)
        copy(2, send, got, partner(t - 1)).start()
        return carry

    lax.fori_loop(early, devices, pick_and_send, 0)
    count_slots(seed_ref, seed_own, seed_near, marks2, 0, 1)
    copy(2, send, got, partner(devices - 1)).start()
    wide = 2 * LANES
    groups = 4 if devices % 4 == 0 else 1
    many = devices // groups
    for g in reversed(range(groups)):
        wait_all(2, send, got, max(1, g * many), (g + 1) * many)
        lay_side_by_side(count1_ref, got, flat, g * many, (g + 1) * many, partner)
        depth = slice(g * many * cap, (g + 1) * many * cap)

        def add_group(c, carry, g=g, depth=depth):
            cols = tile(c, wide)
            for which, matrix in enumerate((own, near)):
                part = dot32(flat[:, depth], matrix[depth, cols])
                sums[which, :, cols] = part if g == groups - 1 else sums[which, :, cols] + part
            return carry

        if g > 0:
            lax.fori_loop(0, own.shape[1] // wide, add_group, 0)
    fan_two, fan_one = float(front_ref.shape[0] - 1), float(seed_ref.shape[0] - 1)

    def nodes_chunk(c, carry):
        cols = tile(c, wide)
        add_group(c, 0)
        mine = sums[0, :, cols].astype(jnp.bfloat16)
        summed = (sums[1, :, cols] / fan_two).astype(jnp.bfloat16)
        preact = dot32(w1s[...], mine) + dot32(w1n[...], summed) + bias1
        hidden = jnp.maximum(preact, 0.0).astype(jnp.bfloat16)
        payload[:, cols] = dot32(w2[...], hidden).astype(jnp.bfloat16)
        return carry

    lax.fori_loop(0, own.shape[1] // wide, nodes_chunk, 0)

    def chosen(asker):
        wanted = asked2[asker]
        select = [
            hits(local_rows(wanted, b * LANES, LANES), node_marks)
            for b in range(payload.shape[1] // LANES)
        ]
        return dot32(payload[...], jnp.concatenate(select, axis=0)).astype(jnp.bfloat16)

    got2[me] = chosen(me)
    send2[partner(1)] = chosen(partner(1))

    def choose_and_send(t, carry):
        send2[partner(t)] = chosen(partner(t))
        copy(3, send2, got2, partner(t - 1)).start()
        return carry

    lax.fori_loop(2, devices, choose_and_send, 0)
    count_slots(seed_ref, seed_own, seed_near, marks2, 1, 2)
    copy(3, send2, got2, partner(devices - 1)).start()
    count_slots(seed_ref, seed_own, seed_near, marks2, 2, devices)
    wait_all(3, send2, got2)
    lay_side_by_side(count2_ref, got2, flat2, 0, devices)
    self_term = dot32(flat2[:half], seed_own[...])
    near_term = dot32(flat2[half:], seed_near[...]) / fan_one
    out_ref[...] = (self_term + near_term)[:classes]


def mask_rows(received, counts, capacity):
    is_live = (jnp.arange(capacity, dtype=jnp.int32)[None, :] < counts[:, None]).reshape(-1)
    flat = received.reshape(-1, received.shape[-1])
    return jnp.where(is_live[:, None], flat, jnp.zeros((), flat.dtype))


def right_product(rows, weight):
    return lax.dot_general(
        rows, weight, (((1,), (1,)), ((), ())), preferred_element_type=jnp.float32
    )


def take_body(
    table_t,
    req_rows,
    count1,
    frontier_list,
    req2_rows,
    count2,
    seed_list,
    w1_self,
    w1_neigh,
    bias1,
    w2_self,
    w2_neigh,
    bias2,
):
    feat_width = table_t.shape[0]
    capacity = req_rows.shape[1]
    table_rows = table_t.T
    picked_rows = jnp.take(
        table_rows,
        lax.all_to_all(req_rows, AXES, split_axis=0, concat_axis=0, tiled=True),
        axis=0,
    )
    received = lax.all_to_all(
        picked_rows, AXES, split_axis=0, concat_axis=0, tiled=True
    )
    flat = mask_rows(received, count1, capacity)
    fanout_two = frontier_list.shape[0] - 1
    front_nodes = frontier_list.shape[1]
    picked = jnp.take(flat, frontier_list.reshape(-1), axis=0).reshape(
        fanout_two + 1, front_nodes, feat_width
    )
    summed = (jnp.sum(picked[1:].astype(jnp.float32), axis=0) / fanout_two).astype(jnp.bfloat16)
    preact = right_product(picked[0], w1_self) + right_product(summed, w1_neigh) + bias1[None, :]
    hidden_rows = jax.nn.relu(preact).astype(jnp.bfloat16)
    cap_two = req2_rows.shape[1]
    payload = jnp.concatenate(
        [right_product(hidden_rows, w2_self), right_product(hidden_rows, w2_neigh)], axis=1
    )
    chosen = jnp.take(
        payload,
        lax.all_to_all(req2_rows, AXES, split_axis=0, concat_axis=0, tiled=True),
        axis=0,
    )
    got_back = lax.all_to_all(chosen, AXES, split_axis=0, concat_axis=0, tiled=True)
    flat_two = mask_rows(got_back, count2, cap_two)
    fanout_one = seed_list.shape[0] - 1
    seed_nodes = seed_list.shape[1]
    picked_two = jnp.take(flat_two, seed_list.reshape(-1), axis=0).reshape(
        fanout_one + 1, seed_nodes, flat_two.shape[1]
    )
    classes = w2_self.shape[0]
    near = jnp.sum(picked_two[1:, :, classes:], axis=0) / fanout_one
    logits = (picked_two[0, :, :classes] + near).T + bias2[:, None]
    return logits


def body(
    table_t,
    req_rows,
    count1,
    frontier_list,
    req2_rows,
    count2,
    seed_list,
    w1_self,
    w1_neigh,
    bias1,
    w2_self,
    w2_neigh,
    bias2,
):
    devices, cap = req_rows.shape
    cap_two = req2_rows.shape[1]
    nodes = frontier_list.shape[1]
    if devices * max(cap, cap_two) * nodes > MATRIX_LIMIT:
        return take_body(
            table_t,
            req_rows,
            count1,
            frontier_list,
            req2_rows,
            count2,
            seed_list,
            w1_self,
            w1_neigh,
            bias1,
            w2_self,
            w2_neigh,
            bias2,
        )
    width, table_rows = table_t.shape
    seeds = seed_list.shape[1]
    hidden_width, classes = w1_self.shape[0], w2_self.shape[0]
    rows_two = 2 * (-(-classes // 16) * 16)
    slots, slots_two = devices * cap, devices * cap_two
    bf16, f32, i32 = jnp.bfloat16, jnp.float32, jnp.int32
    logits = pl.pallas_call(
        functools.partial(whole_kernel, lax.axis_size(AXES[1])),
        in_specs=[pl.BlockSpec(memory_space=pl.ANY)] + [VMEM_ALL] * 2 + [SMEM_ALL] * 2 + [VMEM_ALL] * 7,
        out_specs=VMEM_ALL,
        out_shape=jax.ShapeDtypeStruct((classes, seeds), f32),
        scratch_shapes=[
            pltpu.VMEM((width, table_rows), bf16),
            pltpu.VMEM((hidden_width, width), bf16),
            pltpu.VMEM((hidden_width, width), bf16),
            pltpu.VMEM((rows_two, hidden_width), bf16),
            pltpu.VMEM((devices, 1, cap), i32),
            pltpu.VMEM((devices, 1, cap_two), i32),
            pltpu.SMEM((devices, 1, cap), i32),
            pltpu.VMEM((table_rows, width), f32),
            pltpu.VMEM((cap, width), f32),
            pltpu.VMEM((devices, width, cap), bf16),
            pltpu.VMEM((devices, width, cap), bf16),
            pltpu.VMEM((slots, nodes), bf16),
            pltpu.VMEM((slots, nodes), bf16),
            pltpu.VMEM((slots_two, seeds), bf16),
            pltpu.VMEM((slots_two, seeds), bf16),
            pltpu.VMEM((width, slots), bf16),
            pltpu.VMEM((2, width, nodes), f32),
            pltpu.VMEM((rows_two, nodes), bf16),
            pltpu.VMEM((devices, rows_two, cap_two), bf16),
            pltpu.VMEM((devices, rows_two, cap_two), bf16),
            pltpu.VMEM((rows_two, slots_two), bf16),
            pltpu.SemaphoreType.DMA,
            pltpu.SemaphoreType.DMA,
            pltpu.SemaphoreType.DMA((8, devices)),
        ],
        compiler_params=pltpu.CompilerParams(
            vmem_limit_bytes=63 * MIB, collective_id=0, has_side_effects=True
        ),
    )(
        table_t,
        req_rows[:, None, :],
        req2_rows[:, None, :],
        count1,
        count2,
        frontier_list,
        seed_list,
        w1_self.T,
        w1_neigh.T,
        bias1[None, :],
        w2_self,
        w2_neigh,
    )
    return logits + bias2[:, None]


def solution(mesh):
    in_specs = (
        P(None, AXES),
        P(AXES, None),
        P(AXES),
        P(None, AXES),
        P(AXES, None),
        P(AXES),
        P(None, AXES),
        P(),
        P(),
        P(),
        P(),
        P(),
        P(),
    )
    return jax.shard_map(
        body, mesh=mesh, in_specs=in_specs, out_specs=P(None, AXES), check_vma=False
    )
```
